256 devices in a mesh: group: 4 (over y, x), col: 64 (over z, core).
Axes of the slice: x: 2, y: 2, z: 32, core: 2. Of those that a mesh axis runs over, the one named last changes fastest.
The devices are a block of a 4x8x32 slice.
Arguments:
- homolog_embedding: bfloat16 [384, 256, 256], P('group', 'col'), parts along dimension 0, may hold values from -6 to 6
- left_factor_matrix: bfloat16 [256, 32], replicated, may hold values from -0.375 to 0.375
- right_factor_matrix: bfloat16 [256, 32], replicated, may hold values from -0.375 to 0.375
- decoder: bfloat16 [1024, 128], replicated, may hold values from -2 to 2
- pair_output_bias: float32 [128], replicated, may hold values from -3 to 3
- pair_output_gradient: bfloat16 [1024, 256, 128], P('group', 'col'), parts along dimension 0, may hold values from -16 to 16
Outputs:
- first_operand_gradient: float32 [384, 256, 32], P('group', 'col'), parts along dimension 0
- second_operand_gradient: float32 [384, 256, 32], P('group', 'col'), parts along dimension 0
- alignment_gradient: bfloat16 [384, 256, 256], P('group', 'col'), parts along dimension 0
The draws below stay inside these ranges and needn't reach their ends.
There are 4 independent parts, one for each index of `group`. The reference program is written for one: setup_inputs(seed, part) draws one part's arguments, and reference() takes and returns one part's arrays. A program takes and returns all parts, laid end to end along the dimension named above; an argument that names none is the same for every part. Nothing has to cross between parts.
All inputs are finite; a program needn't handle non-finite values.
Results may differ from the reference program's by a relative error of at most 0.0083.
Values may be sent and summed in bfloat16 or wider, within the bound.
No kernel may reach another device: no remote copies, remote signals or barrier semaphores. Data moves between devices by JAX's collectives and lax.ppermute only.
A program may use at most 64 MiB of HBM per device.

```python
import jax
import jax.numpy as jnp
from jax import lax

EMBED_DEPTH = 256
FACTOR_DEPTH = 32
C_Z = 128
HOMOLOG_TALLY = 96
LOCAL_RESIDUES = 4
POSITION_TALLY = 256


def raised(values, stream_key, source, target, blocks, factor):
    owner, partner = [(jnp.arange(values.shape[position]) // (values.shape[position] // blocks)).reshape([-1 if axis == position else 1 for axis in range(values.ndim)]) for position in (source, target)]
    chosen = jax.random.permutation(stream_key, blocks)[partner]
    strong = (owner == chosen) | (owner == (partner + blocks // 2) % blocks)
    return jnp.where(strong, factor * values, values)


def block_levels(own_key, extent, shards, smallest, largest):
    level = 1.0
    for dim, shards_of in shards:
        steps = jax.random.uniform(jax.random.fold_in(jax.random.fold_in(own_key, 6), dim), (shards_of,), jnp.float32, smallest / len(shards), largest / len(shards))
        level = level * jnp.repeat(jnp.exp(steps), extent[dim] // shards_of).reshape((-1,) + (1,) * (len(extent) - 1 - dim))
    return level


def normal_values(rng, dims, scale, reach, shards=(), dtype=jnp.bfloat16):
    values = scale * jax.random.normal(rng, dims, jnp.float32)
    if shards:
        values = values * block_levels(rng, dims, shards, -0.22, 0.18)
    return jnp.clip(values, -reach, reach).astype(dtype)


def gaussian_with(stream_key, extent, scale, reach, cuts, heavy, kind=jnp.bfloat16):
    entries = scale * jax.random.normal(stream_key, extent, jnp.float32)
    if cuts:
        entries = entries * block_levels(stream_key, extent, cuts, -0.22, 0.18)
    return jnp.clip(raised(entries, jax.random.fold_in(stream_key, 3), *heavy), -reach, reach).astype(kind)


def setup_inputs(seed: int = 0, part: int = 0) -> dict:
    key_list = jax.random.split(jax.random.key(seed), 7)
    part_splits = jax.random.split(jax.random.fold_in(key_list[6], part), 7)
    return {
        "homolog_embedding": normal_values(part_splits[0], (HOMOLOG_TALLY, POSITION_TALLY, EMBED_DEPTH), 1.0, 6.0, ((1, 64),)),
        "left_factor_matrix": normal_values(key_list[1], (EMBED_DEPTH, FACTOR_DEPTH), EMBED_DEPTH ** -0.5, 0.375),
        "right_factor_matrix": normal_values(key_list[2], (EMBED_DEPTH, FACTOR_DEPTH), EMBED_DEPTH ** -0.5, 0.375),
        "decoder": normal_values(key_list[3], (FACTOR_DEPTH * FACTOR_DEPTH, C_Z), (FACTOR_DEPTH * FACTOR_DEPTH // HOMOLOG_TALLY) ** -0.5, 2.0),
        "pair_output_bias": normal_values(key_list[4], (C_Z,), 0.5, 3.0, (), jnp.float32),
        "pair_output_gradient": gaussian_with(part_splits[5], (POSITION_TALLY, POSITION_TALLY, C_Z), 1.0, 16.0, ((1, 64),), (1, 0, 64, 4.0)),
    }


def reference(homolog_embedding, left_factor_matrix, right_factor_matrix, decoder, pair_output_bias, pair_output_gradient):
    alignment_row_count, residue_length, alignment_channel_width = homolog_embedding.shape
    operand_channel_width = left_factor_matrix.shape[1]
    channels = decoder.shape[1]
    reciprocal_rows = 1.0 / alignment_row_count
    alignment_flattened_rows = homolog_embedding.reshape(alignment_row_count * residue_length, alignment_channel_width)
    first_operand_rows = jnp.dot(alignment_flattened_rows, left_factor_matrix, preferred_element_type=jnp.float32).astype(jnp.bfloat16).reshape(alignment_row_count, residue_length, operand_channel_width)
    second_operand_rows = jnp.dot(alignment_flattened_rows, right_factor_matrix, preferred_element_type=jnp.float32).astype(jnp.bfloat16).reshape(alignment_row_count, residue_length, operand_channel_width)
    count_of_blocks = residue_length // LOCAL_RESIDUES
    first_operand_blocks = first_operand_rows.reshape(alignment_row_count, count_of_blocks, LOCAL_RESIDUES, operand_channel_width).transpose(1, 0, 2, 3)
    cot_blocks = pair_output_gradient.reshape(count_of_blocks, LOCAL_RESIDUES, residue_length, channels)
    right_wide = second_operand_rows.astype(jnp.float32)

    def one_block(state_sum, items):
        left_block, upstream = items
        products = jnp.einsum("sic,sjd->ijcd", left_block.astype(jnp.float32), right_wide) * reciprocal_rows
        products = products.astype(jnp.bfloat16).reshape(LOCAL_RESIDUES * residue_length, operand_channel_width * operand_channel_width)
        linear = jnp.dot(products, decoder, preferred_element_type=jnp.float32) + pair_output_bias
        pre_slopes = (upstream.reshape(LOCAL_RESIDUES * residue_length, channels).astype(jnp.float32) * 2.0 * jnp.maximum(linear, 0.0)).astype(jnp.bfloat16)
        backward = jnp.dot(pre_slopes, decoder.T, preferred_element_type=jnp.float32) * reciprocal_rows
        slopes = backward.astype(jnp.bfloat16).reshape(LOCAL_RESIDUES, residue_length, operand_channel_width, operand_channel_width).astype(jnp.float32)
        left_grad = jnp.einsum("ijcd,sjd->sic", slopes, right_wide)
        state_sum = state_sum + jnp.einsum("ijcd,sic->sjd", slopes, left_block.astype(jnp.float32))
        return state_sum, left_grad

    starting_carry = jnp.zeros((alignment_row_count, residue_length, operand_channel_width), jnp.float32)
    second_operand_gradient, first_operand_pieces = lax.scan(one_block, starting_carry, (first_operand_blocks, cot_blocks))
    first_operand_gradient = first_operand_pieces.transpose(1, 0, 2, 3).reshape(alignment_row_count, residue_length, operand_channel_width)
    first_operand_gradient_step = first_operand_gradient.astype(jnp.bfloat16).reshape(alignment_row_count * residue_length, operand_channel_width)
    second_operand_gradient_step = second_operand_gradient.astype(jnp.bfloat16).reshape(alignment_row_count * residue_length, operand_channel_width)
    alignment_gradient = jnp.dot(first_operand_gradient_step, left_factor_matrix.T, preferred_element_type=jnp.float32) + jnp.dot(second_operand_gradient_step, right_factor_matrix.T, preferred_element_type=jnp.float32)
    alignment_gradient = alignment_gradient.astype(jnp.bfloat16).reshape(alignment_row_count, residue_length, alignment_channel_width)
    return first_operand_gradient, second_operand_gradient, alignment_gradient
```

```python
import jax
import jax.numpy as jnp
from jax import lax
from jax.experimental import pallas as pl
from jax.experimental.pallas import tpu as pltpu
from jax.sharding import Mesh
from jax.sharding import PartitionSpec as P

INTERPRET = False


def core_kernel(near_ref, far_low_ref, far_high_ref, mine_ref, mix_ref, bias_ref, up_ref,
                out_ref, all_ref, weight_ref, spread_ref):
    residues, width, rows = mine_ref.shape
    channels = bias_ref.shape[1]
    near = near_ref.shape[0]
    half = far_low_ref.shape[0]
    scale = 1.0 / rows
    all_ref[0:near] = near_ref[...]
    all_ref[near : near + half] = far_low_ref[...]
    all_ref[near + half : near + 2 * half] = far_high_ref[...]
    together = 2
    mix = mix_ref[...]
    for first in range(0, residues, together):
        for k in range(together):
            made = lax.dot_general(
                mine_ref[first + k], mix, (((0,), (0,)), ((), ())),
                preferred_element_type=jnp.float32,
            ).astype(jnp.bfloat16)
            for c in range(width):
                weight_ref[c * rows : (c + 1) * rows, k * channels : (k + 1) * channels] = made[
                    :, c * channels : (c + 1) * channels
                ]
        linear = jnp.dot(all_ref[...], weight_ref[...], preferred_element_type=jnp.float32)
        span = slice(first * channels, (first + together) * channels)
        bias = jnp.concatenate([bias_ref[...]] * together, axis=1)
        slopes = (
            up_ref[:, span].astype(jnp.float32) * 2.0 * jnp.maximum(linear * scale + bias, 0.0)
        ).astype(jnp.bfloat16)
        back = lax.dot_general(
            all_ref[...], slopes, (((0,), (0,)), ((), ())), preferred_element_type=jnp.float32
        ).astype(jnp.bfloat16)
        for k in range(together):
            for c in range(width):
                spread_ref[k * rows : (k + 1) * rows, c * channels : (c + 1) * channels] = back[
                    c * rows : (c + 1) * rows, k * channels : (k + 1) * channels
                ]
        out = lax.dot_general(
            spread_ref[...], mix, (((1,), (1,)), ((), ())), preferred_element_type=jnp.float32
        )
        out_ref[first * rows : (first + together) * rows] = out * scale


def core_call(near, far_low, far_high, mine, mix, bias, up):
    residues, width, rows = mine.shape
    channels = bias.shape[1]
    count = near.shape[0] + far_low.shape[0] + far_high.shape[0]
    return pl.pallas_call(
        core_kernel,
        out_shape=jax.ShapeDtypeStruct((residues * rows, width), jnp.float32),
        scratch_shapes=[
            pltpu.VMEM((count, width * rows), jnp.bfloat16),
            pltpu.VMEM((width * rows, 2 * channels), jnp.bfloat16),
            pltpu.VMEM((2 * rows, width * channels), jnp.bfloat16),
        ],
        compiler_params=pltpu.CompilerParams(vmem_limit_bytes=48 * 1024 * 1024),
        cost_estimate=pl.CostEstimate(flops=4_000_000_000, bytes_accessed=4_000_000, transcendentals=0),
        interpret=INTERPRET,
        name="pair_core",
    )(near, far_low, far_high, mine, mix, bias, up)


def per_device(
    homolog_embedding,
    left_factor_matrix,
    right_factor_matrix,
    decoder,
    pair_output_bias,
    pair_output_gradient,
):
    rows, local, depth = homolog_embedding.shape
    width = left_factor_matrix.shape[1]
    channels = decoder.shape[1]
    total = pair_output_gradient.shape[0]
    high = lax.axis_size("high")
    chips = high * 2
    core = lax.axis_index("core")
    low = lax.axis_index("low")
    z = ("high", "low")
    pair = 2 * local
    swap = [(0, 1), (1, 0)]
    up = [(k, (k + 1) % chips) for k in range(chips)]
    down = [(k, (k - 1) % chips) for k in range(chips)]

    turned = lax.all_to_all(pair_output_gradient, z, 0, 0, tiled=True)

    factors = jnp.concatenate([left_factor_matrix, right_factor_matrix], axis=1)
    operands = jnp.einsum(
        "sje,ek->jks", homolog_embedding, factors, preferred_element_type=jnp.float32
    ).astype(jnp.bfloat16)
    other = lax.ppermute(operands, "core", swap)
    operands = jnp.where(
        core == 0,
        jnp.concatenate([operands, other], axis=0),
        jnp.concatenate([other, operands], axis=0),
    )
    sent = jnp.where(core == 0, operands[:, :width], operands[:, width:])
    mine = jnp.where(core == 0, operands[:, width:], operands[:, :width])
    near = lax.all_gather(sent.reshape(pair, width * rows), "high", axis=0, tiled=True)
    half = near.shape[0] // 2
    far_low = lax.ppermute(near[:half], z, up)
    far_high = lax.ppermute(near[half:], z, down)

    given = jnp.where(core == 0, turned, pair_output_gradient)
    kept = jnp.where(core == 0, pair_output_gradient, turned)
    taken = lax.ppermute(given, "core", swap)
    by_column = jnp.concatenate(
        [kept.reshape(total, local * channels), taken.reshape(total, local * channels)], axis=1
    )

    def across(x):
        return (
            x.reshape(chips, pair, local, channels)
            .transpose(0, 2, 1, 3)
            .reshape(chips, local, pair * channels)
        )

    by_row = jnp.concatenate([across(taken), across(kept)], axis=1).reshape(total, pair * channels)
    upstream = jnp.where(core == 0, by_column, by_row).reshape(high, 2, pair, pair * channels)
    upstream = jnp.where(low == 0, upstream, upstream[:, ::-1])
    upstream = upstream.transpose(1, 0, 2, 3).reshape(total, pair * channels)

    mix = decoder.reshape(width, width, channels)
    mix = jnp.where(core == 0, mix.transpose(1, 0, 2), mix).reshape(width, width * channels)
    gradient = core_call(
        near, far_low, far_high, mine, mix, pair_output_bias.reshape(1, channels), upstream
    ).reshape(2, local, rows, width)
    own = jnp.where(core == 0, gradient[0], gradient[1])
    theirs = lax.ppermute(jnp.where(core == 0, gradient[1], gradient[0]), "core", swap)
    first = jnp.where(core == 0, theirs, own).transpose(1, 0, 2)
    second = jnp.where(core == 0, own, theirs).transpose(1, 0, 2)
    alignment = jnp.einsum(
        "sjk,ek->sje",
        jnp.concatenate([first, second], axis=2).astype(jnp.bfloat16),
        factors,
        preferred_element_type=jnp.float32,
    ).astype(jnp.bfloat16)
    return first, second, alignment


def solution(mesh):
    groups = mesh.shape["group"]
    split = Mesh(
        mesh.devices.reshape(groups, mesh.shape["col"] // 4, 2, 2), ("group", "high", "low", "core")
    )
    tall = P("group", ("high", "low", "core"), None)
    return jax.shard_map(
        per_device,
        mesh=split,
        in_specs=(tall, P(), P(), P(), P(), tall),
        out_specs=(tall, tall, tall),
        check_vma=False,
    )
```

```python
import jax
import jax.numpy as jnp
from jax import lax
from jax.experimental import pallas as pl
from jax.experimental.pallas import tpu as pltpu
from jax.sharding import Mesh
from jax.sharding import PartitionSpec as P


INTERPRET = False
TOGETHER = 2


def build_weight(mine_ref, mix, weight_ref, first):
    _, width, rows = mine_ref.shape
    channels = mix.shape[1] // width
    for k in range(TOGETHER):
        made = lax.dot_general(
            mine_ref[first + k], mix, (((0,), (0,)), ((), ())),
            preferred_element_type=jnp.float32,
        ).astype(jnp.bfloat16)
        for c in range(width):
            weight_ref[c * rows : (c + 1) * rows, k * channels : (k + 1) * channels] = made[
                :, c * channels : (c + 1) * channels
            ]


def slopes_of(linear, scale, bias, upstream):
    return (
        upstream.astype(jnp.float32) * 2.0 * jnp.maximum(linear * scale + bias, 0.0)
    ).astype(jnp.bfloat16)


def pull_back(flipped_ref, slopes, mix_ref, spread_ref, channels):
    width = mix_ref.shape[0]
    rows = flipped_ref.shape[0] // width
    back = jnp.dot(flipped_ref[...], slopes, preferred_element_type=jnp.float32).astype(
        jnp.bfloat16
    )
    for k in range(TOGETHER):
        for c in range(width):
            spread_ref[k * rows : (k + 1) * rows, c * channels : (c + 1) * channels] = back[
                c * rows : (c + 1) * rows, k * channels : (k + 1) * channels
            ]
    out = lax.dot_general(
        spread_ref[...], mix_ref[...], (((1,), (1,)), ((), ())),
        preferred_element_type=jnp.float32,
    )
    return out * (1.0 / rows)


def ahead_kernel(near_ref, far_low_ref, far_high_ref, mine_left_ref, mine_right_ref, by_left_ref,
                 by_right_ref, bias_ref, up_ref, out_ref, linear_ref, flipped_ref, all_ref,
                 weight_ref, spread_ref):
    residues, _, rows = mine_left_ref.shape
    channels = bias_ref.shape[1]
    near = near_ref.shape[0]
    half = far_low_ref.shape[0]
    scale = 1.0 / rows
    all_ref[0:near] = near_ref[...]
    all_ref[near : near + half] = far_low_ref[...]
    all_ref[near + half :] = far_high_ref[...]
    flipped_ref[...] = all_ref[...].T
    bias = jnp.concatenate([bias_ref[...]] * TOGETHER, axis=1)
    for first in range(0, residues, TOGETHER):
        span = slice(first * channels, (first + TOGETHER) * channels)
        build_weight(mine_right_ref, by_right_ref[...], weight_ref, first)
        linear = jnp.dot(all_ref[...], weight_ref[...], preferred_element_type=jnp.float32)
        slopes = slopes_of(linear, scale, bias, up_ref[:, span])
        out_ref[first * rows : (first + TOGETHER) * rows] = pull_back(
            flipped_ref, slopes, by_right_ref, spread_ref, channels
        )
        build_weight(mine_left_ref, by_left_ref[...], weight_ref, first)
        linear_ref[:, span] = jnp.dot(
            all_ref[...], weight_ref[...], preferred_element_type=jnp.float32
        )


def behind_kernel(linear_ref, flipped_ref, by_left_ref, bias_ref, up_ref, out_ref, spread_ref):
    channels = bias_ref.shape[1]
    rows = flipped_ref.shape[0] // by_left_ref.shape[0]
    residues = linear_ref.shape[1] // channels
    bias = jnp.concatenate([bias_ref[...]] * TOGETHER, axis=1)
    for first in range(0, residues, TOGETHER):
        span = slice(first * channels, (first + TOGETHER) * channels)
        slopes = slopes_of(linear_ref[:, span], 1.0 / rows, bias, up_ref[:, span])
        out_ref[first * rows : (first + TOGETHER) * rows] = pull_back(
            flipped_ref, slopes, by_left_ref, spread_ref, channels
        )


def ahead_call(near, far_low, far_high, mine_left, mine_right, by_left, by_right, bias, up):
    residues, width, rows = mine_left.shape
    channels = bias.shape[1]
    count = up.shape[0]
    return pl.pallas_call(
        ahead_kernel,
        out_shape=(
            jax.ShapeDtypeStruct((residues * rows, width), jnp.float32),
            jax.ShapeDtypeStruct((count, residues * channels), jnp.float32),
            jax.ShapeDtypeStruct((width * rows, count), jnp.bfloat16),
        ),
        scratch_shapes=[
            pltpu.VMEM((count, width * rows), jnp.bfloat16),
            pltpu.VMEM((width * rows, TOGETHER * channels), jnp.bfloat16),
            pltpu.VMEM((TOGETHER * rows, width * channels), jnp.bfloat16),
        ],
        compiler_params=pltpu.CompilerParams(vmem_limit_bytes=32 * 1024 * 1024),
        cost_estimate=pl.CostEstimate(
            flops=6_000_000_000, bytes_accessed=4_000_000, transcendentals=0
        ),
        interpret=INTERPRET,
        name="pair_ahead",
    )(near, far_low, far_high, mine_left, mine_right, by_left, by_right, bias, up)


def behind_call(linear, flipped, by_left, bias, up):
    width = by_left.shape[0]
    rows = flipped.shape[0] // width
    channels = bias.shape[1]
    residues = linear.shape[1] // channels
    return pl.pallas_call(
        behind_kernel,
        out_shape=jax.ShapeDtypeStruct((residues * rows, width), jnp.float32),
        scratch_shapes=[pltpu.VMEM((TOGETHER * rows, width * channels), jnp.bfloat16)],
        compiler_params=pltpu.CompilerParams(vmem_limit_bytes=32 * 1024 * 1024),
        cost_estimate=pl.CostEstimate(
            flops=2_000_000_000, bytes_accessed=4_000_000, transcendentals=0
        ),
        interpret=INTERPRET,
        name="pair_behind",
    )(linear, flipped, by_left, bias, up)


def steps(
    homolog_embedding,
    left_factor_matrix,
    right_factor_matrix,
    decoder,
    pair_output_bias,
    pair_output_gradient,
):
    rows, local, _ = homolog_embedding.shape
    width = left_factor_matrix.shape[1]
    channels = decoder.shape[1]
    high = lax.axis_size("high")
    chips = high * 2
    core = lax.axis_index("core")
    low = lax.axis_index("low")
    z = ("high", "low")
    pair = 2 * local
    swap = [(0, 1), (1, 0)]
    up = [(k, (k + 1) % chips) for k in range(chips)]
    down = [(k, (k - 1) % chips) for k in range(chips)]

    factors = jnp.concatenate([left_factor_matrix, right_factor_matrix], axis=1)
    operands = jnp.einsum(
        "sje,ek->jks", homolog_embedding, factors, preferred_element_type=jnp.float32
    ).astype(jnp.bfloat16)
    sent = jnp.concatenate([operands[:, :width], operands[:, width:]], axis=0)
    near = lax.all_gather(sent.reshape(pair, width * rows), "high", axis=0, tiled=True)
    half = near.shape[0] // 2
    far_low = lax.ppermute(near[:half], z, up)
    far_high = lax.ppermute(near[half:], z, down)
    turned = lax.all_to_all(pair_output_gradient, z, 0, 0, tiled=True)

    def in_order(x):
        x = x.reshape(high, 2, pair, pair * channels)
        x = jnp.where(low == 0, x, x[:, ::-1])
        return x.transpose(1, 0, 2, 3).reshape(chips * pair, pair * channels)

    operands, _ = lax.optimization_barrier((operands, near))
    partner = lax.ppermute(operands, "core", swap)
    mine_right = jnp.concatenate([operands[:, width:], partner[:, width:]], axis=0)
    mine_left = jnp.where(
        core == 0,
        jnp.concatenate([operands[:, :width], partner[:, :width]], axis=0),
        jnp.concatenate([partner[:, :width], operands[:, :width]], axis=0),
    )
    gradient = pair_output_gradient.reshape(chips, 2, local, local, channels)
    theirs = lax.ppermute(jnp.where(core == 0, gradient[:, 1], gradient[:, 0]), "core", swap)
    ours = jnp.where(core == 0, gradient[:, 0], gradient[:, 1])
    by_column = jnp.concatenate(
        [
            ours.reshape(chips, local, local * channels),
            theirs.reshape(chips, local, local * channels),
        ],
        axis=2,
    )
    blank = jnp.zeros_like(by_column)
    by_column = in_order(jnp.concatenate([by_column, blank], axis=1))

    by_left = decoder.reshape(width, width * channels)
    by_right = (
        decoder.reshape(width, width, channels).transpose(1, 0, 2).reshape(width, width * channels)
    )
    bias = pair_output_bias.reshape(1, channels)
    second, linear, flipped = ahead_call(
        near, far_low, far_high, mine_left, mine_right, by_left, by_right, bias, by_column
    )
    second = second.reshape(2, local, rows, width)
    second = second[0] + lax.ppermute(second[1], "core", swap)

    by_row = (
        turned.reshape(chips, pair, local, channels)
        .transpose(0, 2, 1, 3)
        .reshape(chips, local, pair * channels)
    )
    by_row = in_order(jnp.concatenate([blank, by_row], axis=1))
    first = behind_call(linear, flipped, by_left, bias, by_row)
    first = first.reshape(2, local, rows, width)
    first = jnp.where(core == 0, first[0], first[1]) + lax.ppermute(
        jnp.where(core == 0, first[1], first[0]), "core", swap
    )
    first = first.transpose(1, 0, 2)
    second = second.transpose(1, 0, 2)
    alignment = jnp.einsum(
        "sjk,ek->sje",
        jnp.concatenate([first, second], axis=2).astype(jnp.bfloat16),
        factors,
        preferred_element_type=jnp.float32,
    ).astype(jnp.bfloat16)
    return first, second, alignment


def solution(mesh):
    groups = mesh.shape["group"]
    split = Mesh(
        mesh.devices.reshape(groups, mesh.shape["col"] // 4, 2, 2), ("group", "high", "low", "core")
    )
    tall = P("group", ("high", "low", "core"), None)
    return jax.shard_map(
        steps,
        mesh=split,
        in_specs=(tall, P(), P(), P(), P(), tall),
        out_specs=(tall, tall, tall),
        check_vma=False,
    )
```

```python
import jax
import jax.numpy as jnp
from jax import lax
from jax.experimental import pallas as pl
from jax.experimental.pallas import tpu as pltpu
from jax.sharding import Mesh
from jax.sharding import PartitionSpec as P


INTERPRET = False
TOGETHER = 2


def build_weight(mine_ref, mix, weight_ref, first):
    _, width, rows = mine_ref.shape
    channels = mix.shape[1] // width
    for k in range(TOGETHER):
        made = lax.dot_general(
            mine_ref[first + k], mix, (((0,), (0,)), ((), ())),
            preferred_element_type=jnp.float32,
        ).astype(jnp.bfloat16)
        for c in range(width):
            weight_ref[c * rows : (c + 1) * rows, k * channels : (k + 1) * channels] = made[
                :, c * channels : (c + 1) * channels
            ]


def slopes_of(linear, scale, bias, upstream):
    return (
        upstream.astype(jnp.float32) * 2.0 * jnp.maximum(linear * scale + bias, 0.0)
    ).astype(jnp.bfloat16)


def regroup(chosen_ref, table_ref, width):
    count = chosen_ref.shape[0]
    rows = chosen_ref.shape[1] // width
    for c in range(width):
        table_ref[c * count : (c + 1) * count] = chosen_ref[:, c * rows : (c + 1) * rows]


def pull_back(slopes, decoder_ref, spread_ref, first, scale):
    count, _ = slopes[0].shape
    width = spread_ref.shape[1] // count
    back = lax.dot_general(
        decoder_ref[...], jnp.concatenate(slopes, axis=0), (((1,), (1,)), ((), ())),
        preferred_element_type=jnp.float32,
    )
    back = (back * scale).astype(jnp.bfloat16)
    for k in range(len(slopes)):
        at = (first + k) * width
        for c in range(width):
            spread_ref[at : at + width, c * count : (c + 1) * count] = back[
                c * width : (c + 1) * width, k * count : (k + 1) * count
            ]


def ahead_kernel(near_ref, far_low_ref, far_high_ref, pick_left_ref, pick_right_ref, mine_left_ref,
                 mine_right_ref, by_left_ref, by_right_ref, decoder_ref, bias_ref, up_ref,
                 out_ref, linear_ref, right_table_ref,
                 all_ref, chosen_ref, other_ref, weight_ref, left_table_ref, spread_ref):
    residues, width, rows = mine_left_ref.shape
    channels = bias_ref.shape[1]
    near = near_ref.shape[0]
    half = far_low_ref.shape[0]
    scale = 1.0 / rows
    all_ref[0:near] = near_ref[...]
    all_ref[near : near + half] = far_low_ref[...]
    all_ref[near + half :] = far_high_ref[...]
    chosen_ref[...] = jnp.dot(
        pick_left_ref[...], all_ref[...], preferred_element_type=jnp.float32
    ).astype(jnp.bfloat16)
    other_ref[...] = jnp.dot(
        pick_right_ref[...], all_ref[...], preferred_element_type=jnp.float32
    ).astype(jnp.bfloat16)
    regroup(chosen_ref, left_table_ref, width)
    regroup(other_ref, right_table_ref, width)
    bias = bias_ref[...]
    for first in range(0, residues, TOGETHER):
        build_weight(mine_right_ref, by_right_ref[...], weight_ref, first)
        linear = jnp.dot(chosen_ref[...], weight_ref[...], preferred_element_type=jnp.float32)
        slopes = [
            slopes_of(
                linear[:, k * channels : (k + 1) * channels], scale, bias,
                up_ref[:, (first + k) * channels : (first + k + 1) * channels],
            )
            for k in range(TOGETHER)
        ]
        pull_back(slopes, decoder_ref, spread_ref, first, scale)
        build_weight(mine_left_ref, by_left_ref[...], weight_ref, first)
        linear_ref[:, first * channels : (first + TOGETHER) * channels] = jnp.dot(
            other_ref[...], weight_ref[...], preferred_element_type=jnp.float32
        )
    out_ref[...] = jnp.dot(
        spread_ref[...], left_table_ref[...], preferred_element_type=jnp.float32
    )


def behind_kernel(linear_ref, right_table_ref, decoder_ref, bias_ref, up_ref, out_ref, spread_ref):
    channels = bias_ref.shape[1]
    rows = right_table_ref.shape[1]
    residues = linear_ref.shape[1] // channels
    scale = 1.0 / rows
    for first in range(0, residues, TOGETHER):
        slopes = []
        for k in range(TOGETHER):
            span = slice((first + k) * channels, (first + k + 1) * channels)
            slopes.append(slopes_of(linear_ref[:, span], scale, bias_ref[...], up_ref[:, span]))
        pull_back(slopes, decoder_ref, spread_ref, first, scale)
    out_ref[...] = jnp.dot(
        spread_ref[...], right_table_ref[...], preferred_element_type=jnp.float32
    )


def ahead_call(near, far_low, far_high, pick_left, pick_right, mine_left, mine_right, by_left,
               by_right, decoder, bias, up):
    residues, width, rows = mine_left.shape
    channels = bias.shape[1]
    count, wide = pick_left.shape
    return pl.pallas_call(
        ahead_kernel,
        out_shape=(
            jax.ShapeDtypeStruct((residues * width, rows), jnp.float32),
            jax.ShapeDtypeStruct((count, residues * channels), jnp.float32),
            jax.ShapeDtypeStruct((width * count, rows), jnp.bfloat16),
        ),
        scratch_shapes=[
            pltpu.VMEM((wide, width * rows), jnp.bfloat16),
            pltpu.VMEM((count, width * rows), jnp.bfloat16),
            pltpu.VMEM((count, width * rows), jnp.bfloat16),
            pltpu.VMEM((width * rows, TOGETHER * channels), jnp.bfloat16),
            pltpu.VMEM((width * count, rows), jnp.bfloat16),
            pltpu.VMEM((residues * width, width * count), jnp.bfloat16),
        ],
        compiler_params=pltpu.CompilerParams(vmem_limit_bytes=32 * 1024 * 1024),
        cost_estimate=pl.CostEstimate(
            flops=6_000_000_000, bytes_accessed=4_000_000, transcendentals=0
        ),
        interpret=INTERPRET,
        name="pair_ahead",
    )(near, far_low, far_high, pick_left, pick_right, mine_left, mine_right, by_left, by_right,
      decoder, bias, up)


def behind_call(linear, right_table, decoder, bias, up):
    count = linear.shape[0]
    width = right_table.shape[0] // count
    rows = right_table.shape[1]
    residues = linear.shape[1] // bias.shape[1]
    return pl.pallas_call(
        behind_kernel,
        out_shape=jax.ShapeDtypeStruct((residues * width, rows), jnp.float32),
        scratch_shapes=[pltpu.VMEM((residues * width, width * count), jnp.bfloat16)],
        compiler_params=pltpu.CompilerParams(vmem_limit_bytes=16 * 1024 * 1024),
        cost_estimate=pl.CostEstimate(
            flops=2_000_000_000, bytes_accessed=4_000_000, transcendentals=0
        ),
        interpret=INTERPRET,
        name="pair_behind",
    )(linear, right_table, decoder, bias, up)


def steps(
    homolog_embedding,
    left_factor_matrix,
    right_factor_matrix,
    decoder,
    pair_output_bias,
    pair_output_gradient,
):
    rows, local, _ = homolog_embedding.shape
    width = left_factor_matrix.shape[1]
    channels = decoder.shape[1]
    high = lax.axis_size("high")
    chips = high * 2
    core = lax.axis_index("core")
    low = lax.axis_index("low")
    z = ("high", "low")
    pair = 2 * local
    swap = [(0, 1), (1, 0)]
    up = [(k, (k + 1) % chips) for k in range(chips)]
    down = [(k, (k - 1) % chips) for k in range(chips)]

    factors = jnp.concatenate([left_factor_matrix, right_factor_matrix], axis=1)
    operands = jnp.einsum(
        "sje,ek->jks", homolog_embedding, factors, preferred_element_type=jnp.float32
    ).astype(jnp.bfloat16)
    sent = jnp.concatenate([operands[:, :width], operands[:, width:]], axis=0)
    near = lax.all_gather(sent.reshape(pair, width * rows), "high", axis=0, tiled=True)
    half = near.shape[0] // 2
    far_low = lax.ppermute(near[:half], z, up)
    far_high = lax.ppermute(near[half:], z, down)
    turned = lax.all_to_all(pair_output_gradient, z, 0, 0, tiled=True)

    def pick(offset):
        row = lax.broadcasted_iota(jnp.int32, (chips * local, chips * pair), 0)
        column = lax.broadcasted_iota(jnp.int32, (chips * local, chips * pair), 1)
        chip = row // local
        source = (chip // 2) * pair + offset * local + row % local
        source = source + jnp.where(chip % 2 == low, 0, high * pair)
        return (column == source).astype(jnp.bfloat16)

    operands, _ = lax.optimization_barrier((operands, near))
    partner = lax.ppermute(operands, "core", swap)
    mine_right = jnp.concatenate([operands[:, width:], partner[:, width:]], axis=0)
    mine_left = jnp.where(
        core == 0,
        jnp.concatenate([operands[:, :width], partner[:, :width]], axis=0),
        jnp.concatenate([partner[:, :width], operands[:, :width]], axis=0),
    )
    gradient = pair_output_gradient.reshape(chips, 2, local, local, channels)
    theirs = lax.ppermute(jnp.where(core == 0, gradient[:, 1], gradient[:, 0]), "core", swap)
    ours = jnp.where(core == 0, gradient[:, 0], gradient[:, 1])
    by_column = jnp.concatenate(
        [
            ours.reshape(chips, local, local * channels),
            theirs.reshape(chips, local, local * channels),
        ],
        axis=2,
    )
    by_column = by_column.reshape(chips * local, pair * channels)

    by_left = decoder.reshape(width, width * channels)
    by_right = (
        decoder.reshape(width, width, channels).transpose(1, 0, 2).reshape(width, width * channels)
    )
    bias = pair_output_bias.reshape(1, channels)
    second, linear, right_table = ahead_call(
        near, far_low, far_high, pick(0), pick(1), mine_left, mine_right, by_left, by_right,
        decoder, bias, by_column,
    )
    second = second.reshape(2, local, width, rows)
    second = second[0] + lax.ppermute(second[1], "core", swap)

    by_row = (
        turned.reshape(chips, pair, local, channels)
        .transpose(0, 2, 1, 3)
        .reshape(chips * local, pair * channels)
    )
    first = behind_call(
        linear, right_table, by_right.reshape(decoder.shape), bias, by_row
    )
    first = first.reshape(2, local, width, rows)
    first = jnp.where(core == 0, first[0], first[1]) + lax.ppermute(
        jnp.where(core == 0, first[1], first[0]), "core", swap
    )
    alignment = jnp.einsum(
        "jks,ek->sje",
        jnp.concatenate([first, second], axis=1).astype(jnp.bfloat16),
        factors,
        preferred_element_type=jnp.float32,
    ).astype(jnp.bfloat16)
    return first.transpose(2, 0, 1), second.transpose(2, 0, 1), alignment


def solution(mesh):
    groups = mesh.shape["group"]
    split = Mesh(
        mesh.devices.reshape(groups, mesh.shape["col"] // 4, 2, 2), ("group", "high", "low", "core")
    )
    tall = P("group", ("high", "low", "core"), None)
    return jax.shard_map(
        steps,
        mesh=split,
        in_specs=(tall, P(), P(), P(), P(), tall),
        out_specs=(tall, tall, tall),
        check_vma=False,
    )
```

```python
import jax
import jax.numpy as jnp
from jax import lax
from jax.experimental import pallas as pl
from jax.experimental.pallas import tpu as pltpu
from jax.sharding import Mesh
from jax.sharding import PartitionSpec as P


INTERPRET = False
TOGETHER = 2


def slopes_of(linear, bias, upstream):
    return (upstream.astype(jnp.float32) * 2.0 * jnp.maximum(linear + bias, 0.0)).astype(
        jnp.bfloat16
    )


def push_forward(mine, table_ref, decoder_ref, spread_ref, width, scale):
    count = table_ref.shape[0] // width
    made = lax.dot_general(
        mine, table_ref[...], (((1,), (1,)), ((), ())), preferred_element_type=jnp.float32
    )
    made = (made * scale).astype(jnp.bfloat16)
    for k in range(mine.shape[0] // width):
        for c in range(width):
            spread_ref[c * width : (c + 1) * width, k * count : (k + 1) * count] = made[
                k * width : (k + 1) * width, c * count : (c + 1) * count
            ]
    return lax.dot_general(
        decoder_ref[...], spread_ref[...], (((0,), (0,)), ((), ())),
        preferred_element_type=jnp.float32,
    )


def regroup(chosen_ref, table_ref, width):
    count = chosen_ref.shape[0]
    rows = chosen_ref.shape[1] // width
    for c in range(width):
        table_ref[c * count : (c + 1) * count] = chosen_ref[:, c * rows : (c + 1) * rows]


def pull_back(slopes, decoder_ref, spread_ref, first, scale):
    count, _ = slopes[0].shape
    width = spread_ref.shape[1] // count
    back = lax.dot_general(
        decoder_ref[...], jnp.concatenate(slopes, axis=0), (((1,), (1,)), ((), ())),
        preferred_element_type=jnp.float32,
    )
    back = (back * scale).astype(jnp.bfloat16)
    for k in range(len(slopes)):
        at = (first + k) * width
        for c in range(width):
            spread_ref[at : at + width, c * count : (c + 1) * count] = back[
                c * width : (c + 1) * width, k * count : (k + 1) * count
            ]


def ahead_kernel(near_ref, far_low_ref, far_high_ref, pick_left_ref, pick_right_ref, mine_left_ref,
                 mine_right_ref, decoder_ref, turned_decoder_ref, bias_ref, up_ref,
                 out_ref, linear_ref, right_table_ref,
                 all_ref, chosen_ref, left_table_ref, product_ref, spread_ref):
    residues, width, rows = mine_left_ref.shape
    channels = bias_ref.shape[1]
    count = up_ref.shape[0]
    near = near_ref.shape[0]
    half = far_low_ref.shape[0]
    scale = 1.0 / rows
    all_ref[0:near] = near_ref[...]
    all_ref[near : near + half] = far_low_ref[...]
    all_ref[near + half :] = far_high_ref[...]
    for pick_ref, table_ref in ((pick_left_ref, left_table_ref), (pick_right_ref, right_table_ref)):
        chosen_ref[...] = jnp.dot(
            pick_ref[...], all_ref[...], preferred_element_type=jnp.float32
        ).astype(jnp.bfloat16)
        regroup(chosen_ref, table_ref, width)
    linear = push_forward(
        mine_right_ref[...].reshape(residues * width, rows), left_table_ref, decoder_ref,
        product_ref, width, scale,
    )
    for first in range(0, residues, TOGETHER):
        slopes = [
            slopes_of(
                linear[:, k * count : (k + 1) * count].T, bias_ref[...],
                up_ref[:, k * channels : (k + 1) * channels],
            )
            for k in range(first, first + TOGETHER)
        ]
        pull_back(slopes, decoder_ref, spread_ref, first, scale)
    out_ref[...] = jnp.dot(
        spread_ref[...], left_table_ref[...], preferred_element_type=jnp.float32
    )
    linear = push_forward(
        mine_left_ref[...].reshape(residues * width, rows), right_table_ref, turned_decoder_ref,
        product_ref, width, scale,
    )
    for k in range(residues):
        linear_ref[:, k * channels : (k + 1) * channels] = linear[:, k * count : (k + 1) * count].T


def behind_kernel(linear_ref, right_table_ref, decoder_ref, bias_ref, up_ref, out_ref, spread_ref):
    channels = bias_ref.shape[1]
    rows = right_table_ref.shape[1]
    residues = linear_ref.shape[1] // channels
    scale = 1.0 / rows
    for first in range(0, residues, TOGETHER):
        slopes = []
        for k in range(TOGETHER):
            span = slice((first + k) * channels, (first + k + 1) * channels)
            slopes.append(slopes_of(linear_ref[:, span], bias_ref[...], up_ref[:, span]))
        pull_back(slopes, decoder_ref, spread_ref, first, scale)
    out_ref[...] = jnp.dot(
        spread_ref[...], right_table_ref[...], preferred_element_type=jnp.float32
    )


def ahead_call(near, far_low, far_high, pick_left, pick_right, mine_left, mine_right, decoder,
               turned_decoder, bias, up):
    residues, width, rows = mine_left.shape
    channels = bias.shape[1]
    count, wide = pick_left.shape
    return pl.pallas_call(
        ahead_kernel,
        out_shape=(
            jax.ShapeDtypeStruct((residues * width, rows), jnp.float32),
            jax.ShapeDtypeStruct((count, residues * channels), jnp.float32),
            jax.ShapeDtypeStruct((width * count, rows), jnp.bfloat16),
        ),
        scratch_shapes=[
            pltpu.VMEM((wide, width * rows), jnp.bfloat16),
            pltpu.VMEM((count, width * rows), jnp.bfloat16),
            pltpu.VMEM((width * count, rows), jnp.bfloat16),
            pltpu.VMEM((width * width, residues * count), jnp.bfloat16),
            pltpu.VMEM((residues * width, width * count), jnp.bfloat16),
        ],
        compiler_params=pltpu.CompilerParams(vmem_limit_bytes=32 * 1024 * 1024),
        cost_estimate=pl.CostEstimate(
            flops=3_000_000_000, bytes_accessed=4_000_000, transcendentals=0
        ),
        interpret=INTERPRET,
        name="pair_ahead",
    )(near, far_low, far_high, pick_left, pick_right, mine_left, mine_right, decoder,
      turned_decoder, bias, up)


def behind_call(linear, right_table, decoder, bias, up):
    count = linear.shape[0]
    width = right_table.shape[0] // count
    rows = right_table.shape[1]
    residues = linear.shape[1] // bias.shape[1]
    return pl.pallas_call(
        behind_kernel,
        out_shape=jax.ShapeDtypeStruct((residues * width, rows), jnp.float32),
        scratch_shapes=[pltpu.VMEM((residues * width, width * count), jnp.bfloat16)],
        compiler_params=pltpu.CompilerParams(vmem_limit_bytes=16 * 1024 * 1024),
        cost_estimate=pl.CostEstimate(
            flops=2_000_000_000, bytes_accessed=4_000_000, transcendentals=0
        ),
        interpret=INTERPRET,
        name="pair_behind",
    )(linear, right_table, decoder, bias, up)


def steps(
    homolog_embedding,
    left_factor_matrix,
    right_factor_matrix,
    decoder,
    pair_output_bias,
    pair_output_gradient,
):
    rows, local, _ = homolog_embedding.shape
    width = left_factor_matrix.shape[1]
    channels = decoder.shape[1]
    high = lax.axis_size("high")
    chips = high * 2
    core = lax.axis_index("core")
    low = lax.axis_index("low")
    z = ("high", "low")
    pair = 2 * local
    swap = [(0, 1), (1, 0)]
    up = [(k, (k + 1) % chips) for k in range(chips)]
    down = [(k, (k - 1) % chips) for k in range(chips)]

    factors = jnp.concatenate([left_factor_matrix, right_factor_matrix], axis=1)
    operands = jnp.einsum(
        "sje,ek->jks", homolog_embedding, factors, preferred_element_type=jnp.float32
    ).astype(jnp.bfloat16)
    sent = jnp.concatenate([operands[:, :width], operands[:, width:]], axis=0)
    near = lax.all_gather(sent.reshape(pair, width * rows), "high", axis=0, tiled=True)
    half = near.shape[0] // 2
    far_low = lax.ppermute(near[:half], z, up)
    far_high = lax.ppermute(near[half:], z, down)
    turned = lax.all_to_all(pair_output_gradient, z, 0, 0, tiled=True)

    def pick(offset):
        row = lax.broadcasted_iota(jnp.int32, (chips * local, chips * pair), 0)
        column = lax.broadcasted_iota(jnp.int32, (chips * local, chips * pair), 1)
        chip = row // local
        source = (chip // 2) * pair + offset * local + row % local
        source = source + jnp.where(chip % 2 == low, 0, high * pair)
        return (column == source).astype(jnp.bfloat16)

    operands, _ = lax.optimization_barrier((operands, near))
    partner = lax.ppermute(operands, "core", swap)
    mine_right = jnp.concatenate([operands[:, width:], partner[:, width:]], axis=0)
    mine_left = jnp.where(
        core == 0,
        jnp.concatenate([operands[:, :width], partner[:, :width]], axis=0),
        jnp.concatenate([partner[:, :width], operands[:, :width]], axis=0),
    )
    gradient = pair_output_gradient.reshape(chips, 2, local, local, channels)
    theirs = lax.ppermute(jnp.where(core == 0, gradient[:, 1], gradient[:, 0]), "core", swap)
    ours = jnp.where(core == 0, gradient[:, 0], gradient[:, 1])
    by_column = jnp.concatenate(
        [
            ours.reshape(chips, local, local * channels),
            theirs.reshape(chips, local, local * channels),
        ],
        axis=2,
    )
    by_column = by_column.reshape(chips * local, pair * channels)

    turned_decoder = (
        decoder.reshape(width, width, channels).transpose(1, 0, 2).reshape(decoder.shape)
    )
    bias = pair_output_bias.reshape(1, channels)
    second, linear, right_table = ahead_call(
        near, far_low, far_high, pick(0), pick(1), mine_left, mine_right, decoder,
        turned_decoder, bias, by_column,
    )
    second = second.reshape(2, local, width, rows)
    second = second[0] + lax.ppermute(second[1], "core", swap)

    by_row = (
        turned.reshape(chips, pair, local, channels)
        .transpose(0, 2, 1, 3)
        .reshape(chips * local, pair * channels)
    )
    first = behind_call(
        linear, right_table, turned_decoder, bias, by_row
    )
    first = first.reshape(2, local, width, rows)
    first = jnp.where(core == 0, first[0], first[1]) + lax.ppermute(
        jnp.where(core == 0, first[1], first[0]), "core", swap
    )
    alignment = jnp.einsum(
        "jks,ek->sje",
        jnp.concatenate([first, second], axis=1).astype(jnp.bfloat16),
        factors,
        preferred_element_type=jnp.float32,
    ).astype(jnp.bfloat16)
    return first.transpose(2, 0, 1), second.transpose(2, 0, 1), alignment


def solution(mesh):
    groups = mesh.shape["group"]
    split = Mesh(
        mesh.devices.reshape(groups, mesh.shape["col"] // 4, 2, 2), ("group", "high", "low", "core")
    )
    tall = P("group", ("high", "low", "core"), None)
    return jax.shard_map(
        steps,
        mesh=split,
        in_specs=(tall, P(), P(), P(), P(), tall),
        out_specs=(tall, tall, tall),
        check_vma=False,
    )
```

```python
import jax
import jax.numpy as jnp
from jax import lax
from jax.experimental import pallas as pl
from jax.experimental.pallas import tpu as pltpu
from jax.sharding import Mesh
from jax.sharding import PartitionSpec as P


INTERPRET = False
TOGETHER = 2


def slopes_of(linear, bias, upstream):
    return (upstream.astype(jnp.float32) * 2.0 * jnp.maximum(linear + bias, 0.0)).astype(
        jnp.bfloat16
    )


def push_forward(mine, table_ref, decoder_ref, spread_ref, width, scale):
    count = table_ref.shape[0] // width
    made = lax.dot_general(
        mine, table_ref[...], (((1,), (1,)), ((), ())), preferred_element_type=jnp.float32
    )
    made = (made * scale).astype(jnp.bfloat16)
    for k in range(mine.shape[0] // width):
        for c in range(width):
            spread_ref[c * width : (c + 1) * width, k * count : (k + 1) * count] = made[
                k * width : (k + 1) * width, c * count : (c + 1) * count
            ]
    return lax.dot_general(
        decoder_ref[...], spread_ref[...], (((0,), (0,)), ((), ())),
        preferred_element_type=jnp.float32,
    )


def regroup(chosen_ref, table_ref, width):
    count = chosen_ref.shape[0]
    rows = chosen_ref.shape[1] // width
    for c in range(width):
        table_ref[c * count : (c + 1) * count] = chosen_ref[:, c * rows : (c + 1) * rows]


def pull_back(slopes, decoder_ref, spread_ref, first, scale):
    count, _ = slopes[0].shape
    width = spread_ref.shape[1] // count
    back = lax.dot_general(
        decoder_ref[...], jnp.concatenate(slopes, axis=0), (((1,), (1,)), ((), ())),
        preferred_element_type=jnp.float32,
    )
    back = (back * scale).astype(jnp.bfloat16)
    for k in range(len(slopes)):
        at = (first + k) * width
        for c in range(width):
            spread_ref[at : at + width, c * count : (c + 1) * count] = back[
                c * width : (c + 1) * width, k * count : (k + 1) * count
            ]


def ahead_kernel(near_ref, far_low_ref, far_high_ref, pick_left_ref, pick_right_ref, mine_left_ref,
                 mine_right_ref, decoder_ref, turned_decoder_ref, bias_ref, up_ref,
                 out_ref, linear_ref, right_table_ref,
                 all_ref, chosen_ref, left_table_ref, product_ref, spread_ref):
    residues, width, rows = mine_left_ref.shape
    channels = bias_ref.shape[1]
    count = up_ref.shape[0]
    near = near_ref.shape[0]
    half = far_low_ref.shape[0]
    scale = 1.0 / rows
    all_ref[0:near] = near_ref[...]
    all_ref[near : near + half] = far_low_ref[...]
    all_ref[near + half :] = far_high_ref[...]
    for pick_ref, table_ref in ((pick_left_ref, left_table_ref), (pick_right_ref, right_table_ref)):
        chosen_ref[...] = jnp.dot(
            pick_ref[...], all_ref[...], preferred_element_type=jnp.float32
        ).astype(jnp.bfloat16)
        regroup(chosen_ref, table_ref, width)
    linear = push_forward(
        mine_right_ref[...].reshape(residues * width, rows), left_table_ref, decoder_ref,
        product_ref, width, scale,
    )
    for first in range(0, residues, TOGETHER):
        slopes = [
            slopes_of(
                linear[:, k * count : (k + 1) * count].T, bias_ref[...],
                up_ref[:, k * channels : (k + 1) * channels],
            )
            for k in range(first, first + TOGETHER)
        ]
        pull_back(slopes, decoder_ref, spread_ref, first, scale)
    out_ref[...] = jnp.dot(
        spread_ref[...], left_table_ref[...], preferred_element_type=jnp.float32
    )
    linear = push_forward(
        mine_left_ref[...].reshape(residues * width, rows), right_table_ref, turned_decoder_ref,
        product_ref, width, scale,
    )
    for k in range(residues):
        linear_ref[:, k * channels : (k + 1) * channels] = linear[:, k * count : (k + 1) * count].T


def behind_kernel(linear_ref, right_table_ref, decoder_ref, bias_ref, up_ref, out_ref, spread_ref):
    channels = bias_ref.shape[1]
    rows = right_table_ref.shape[1]
    residues = linear_ref.shape[1] // channels
    scale = 1.0 / rows
    for first in range(0, residues, TOGETHER):
        slopes = []
        for k in range(TOGETHER):
            span = slice((first + k) * channels, (first + k + 1) * channels)
            slopes.append(slopes_of(
                linear_ref[:, span], bias_ref[...],
                up_ref[:, first + k].reshape(linear_ref.shape[0], channels),
            ))
        pull_back(slopes, decoder_ref, spread_ref, first, scale)
    out_ref[...] = jnp.dot(
        spread_ref[...], right_table_ref[...], preferred_element_type=jnp.float32
    )


def ahead_call(near, far_low, far_high, pick_left, pick_right, mine_left, mine_right, decoder,
               turned_decoder, bias, up):
    residues, width, rows = mine_left.shape
    channels = bias.shape[1]
    count, wide = pick_left.shape
    return pl.pallas_call(
        ahead_kernel,
        out_shape=(
            jax.ShapeDtypeStruct((residues * width, rows), jnp.float32),
            jax.ShapeDtypeStruct((count, residues * channels), jnp.float32),
            jax.ShapeDtypeStruct((width * count, rows), jnp.bfloat16),
        ),
        scratch_shapes=[
            pltpu.VMEM((wide, width * rows), jnp.bfloat16),
            pltpu.VMEM((count, width * rows), jnp.bfloat16),
            pltpu.VMEM((width * count, rows), jnp.bfloat16),
            pltpu.VMEM((width * width, residues * count), jnp.bfloat16),
            pltpu.VMEM((residues * width, width * count), jnp.bfloat16),
        ],
        compiler_params=pltpu.CompilerParams(vmem_limit_bytes=32 * 1024 * 1024),
        cost_estimate=pl.CostEstimate(
            flops=3_000_000_000, bytes_accessed=4_000_000, transcendentals=0
        ),
        interpret=INTERPRET,
        name="pair_ahead",
    )(near, far_low, far_high, pick_left, pick_right, mine_left, mine_right, decoder,
      turned_decoder, bias, up)


def behind_call(linear, right_table, decoder, bias, up):
    count = linear.shape[0]
    width = right_table.shape[0] // count
    rows = right_table.shape[1]
    residues = linear.shape[1] // bias.shape[1]
    return pl.pallas_call(
        behind_kernel,
        out_shape=jax.ShapeDtypeStruct((residues * width, rows), jnp.float32),
        scratch_shapes=[pltpu.VMEM((residues * width, width * count), jnp.bfloat16)],
        compiler_params=pltpu.CompilerParams(vmem_limit_bytes=16 * 1024 * 1024),
        cost_estimate=pl.CostEstimate(
            flops=2_000_000_000, bytes_accessed=4_000_000, transcendentals=0
        ),
        interpret=INTERPRET,
        name="pair_behind",
    )(linear, right_table, decoder, bias, up)


def steps(
    homolog_embedding,
    left_factor_matrix,
    right_factor_matrix,
    decoder,
    pair_output_bias,
    pair_output_gradient,
):
    rows, local, _ = homolog_embedding.shape
    width = left_factor_matrix.shape[1]
    channels = decoder.shape[1]
    high = lax.axis_size("high")
    chips = high * 2
    core = lax.axis_index("core")
    low = lax.axis_index("low")
    z = ("high", "low")
    pair = 2 * local
    swap = [(0, 1), (1, 0)]
    up = [(k, (k + 1) % chips) for k in range(chips)]
    down = [(k, (k - 1) % chips) for k in range(chips)]

    factors = jnp.concatenate([left_factor_matrix, right_factor_matrix], axis=1)
    operands = jnp.einsum(
        "sje,ek->jks", homolog_embedding, factors, preferred_element_type=jnp.float32
    ).astype(jnp.bfloat16)
    sent = jnp.concatenate([operands[:, :width], operands[:, width:]], axis=0)
    near = lax.all_gather(sent.reshape(pair, width * rows), "high", axis=0, tiled=True)
    half = near.shape[0] // 2
    far_low = lax.ppermute(near[:half], z, up)
    far_high = lax.ppermute(near[half:], z, down)
    turned = lax.all_to_all(pair_output_gradient, z, 0, 0, tiled=True)

    def pick(offset):
        row = lax.broadcasted_iota(jnp.int32, (chips * local, chips * pair), 0)
        column = lax.broadcasted_iota(jnp.int32, (chips * local, chips * pair), 1)
        chip = row // local
        source = (chip // 2) * pair + offset * local + row % local
        source = source + jnp.where(chip % 2 == low, 0, high * pair)
        return (column == source).astype(jnp.bfloat16)

    operands, _ = lax.optimization_barrier((operands, near))
    partner = lax.ppermute(operands, "core", swap)
    mine_right = jnp.concatenate([operands[:, width:], partner[:, width:]], axis=0)
    mine_left = jnp.where(
        core == 0,
        jnp.concatenate([operands[:, :width], partner[:, :width]], axis=0),
        jnp.concatenate([partner[:, :width], operands[:, :width]], axis=0),
    )
    gradient = pair_output_gradient.reshape(chips, 2, local, local, channels)
    theirs = lax.ppermute(jnp.where(core == 0, gradient[:, 1], gradient[:, 0]), "core", swap)
    ours = jnp.where(core == 0, gradient[:, 0], gradient[:, 1])
    by_column = jnp.concatenate(
        [
            ours.reshape(chips, local, local * channels),
            theirs.reshape(chips, local, local * channels),
        ],
        axis=2,
    )
    by_column = by_column.reshape(chips * local, pair * channels)

    turned_decoder = (
        decoder.reshape(width, width, channels).transpose(1, 0, 2).reshape(decoder.shape)
    )
    bias = pair_output_bias.reshape(1, channels)
    second, linear, right_table = ahead_call(
        near, far_low, far_high, pick(0), pick(1), mine_left, mine_right, decoder,
        turned_decoder, bias, by_column,
    )
    by_row = turned.reshape(chips, pair, local, channels)
    first = behind_call(
        linear, right_table, turned_decoder, bias, by_row
    )
    first, second = lax.optimization_barrier((first, second))
    first = first.reshape(2, local, width, rows)
    second = second.reshape(2, local, width, rows)
    got = lax.ppermute(
        jnp.concatenate([jnp.where(core == 0, first[1], first[0]), second[1]], axis=0),
        "core",
        swap,
    )
    first = jnp.where(core == 0, first[0], first[1]) + got[:local]
    second = second[0] + got[local:]
    alignment = jnp.einsum(
        "jks,ek->sje",
        jnp.concatenate([first, second], axis=1).astype(jnp.bfloat16),
        factors,
        preferred_element_type=jnp.float32,
    ).astype(jnp.bfloat16)
    return first.transpose(2, 0, 1), second.transpose(2, 0, 1), alignment


def solution(mesh):
    groups = mesh.shape["group"]
    split = Mesh(
        mesh.devices.reshape(groups, mesh.shape["col"] // 4, 2, 2), ("group", "high", "low", "core")
    )
    tall = P("group", ("high", "low", "core"), None)
    return jax.shard_map(
        steps,
        mesh=split,
        in_specs=(tall, P(), P(), P(), P(), tall),
        out_specs=(tall, tall, tall),
        check_vma=False,
    )
```
